32 devices in a mesh: dp: 16 (over z, y, core), tensor: 2 (over x).
Axes of the slice: x: 2, y: 2, z: 4, core: 2. Of those that a mesh axis runs over, the one named last changes fastest.
Arguments:
- activations: bfloat16 [4096, 27648], P('dp', 'tensor'), may hold values from -6 to 6
- output_gradient: bfloat16 [4096, 5120], P('dp', 'tensor'), may hold values from -6 to 6
- adapter_a: bfloat16 [2, 13824, 128], P('tensor', 'dp'), may hold values from -0.0390625 to 0.0390625
- adapter_b: bfloat16 [128, 5120], P(None, 'tensor'), may hold values from -0.078125 to 0.078125
- log_ratio: float32 [4096], P('dp'), may hold values from -1.5 to 1.5
- lengths: int32 [1, 16], replicated, may hold values from 1 to 256, as said below
- rewards: int32 [1, 16], replicated, may hold values from 0 to 10
Outputs:
- grad_a: float32 [2, 13824, 128], P('tensor', 'dp')
- adapter_b_gradient: float32 [128, 5120], P(None, 'tensor')
- loss: float32 [], replicated
The draws below stay inside these ranges and needn't reach their ends.
Inputs may be any that keep to these rules, and one draw needn't show every extreme that they name: `lengths`: in every group some rollout has length 256.
All inputs are finite; a program needn't handle non-finite values.
Results may differ from the reference program's by a relative error of at most 0.0067.
Values may be sent and summed in bfloat16 or wider, within the bound.
A program may use at most 64 MiB of HBM per device.

```python
import jax
import jax.numpy as jnp
from jax import lax

D = 5120
FF = 27648
R = 128
ROLLOUTS = 16
MOST = 256
GROUPS = 1
TOKENS = 4096
TP_BLOCKS = 2
FF_TP = 13824


def draw_lengths(key, part):
    first_key, second_key = jax.random.split(jax.random.fold_in(key, 17))
    base = jax.random.randint(first_key, (GROUPS, ROLLOUTS), 1, MOST + 1)
    chosen = jax.random.randint(second_key, (GROUPS, 1), 0, ROLLOUTS)
    column_ids = jnp.arange(ROLLOUTS)[None, :]
    return jnp.where(column_ids == chosen, MOST, base).astype(jnp.int32)


def with_ends(drawn, rng, low, largest):
    shape = drawn.shape
    place = [jax.random.randint(jax.random.fold_in(rng, axis), (), 0, shape[axis]) for axis in range(len(shape))]
    drawn = drawn.at[tuple(place)].set(low)
    longest = shape.index(max(shape))
    place[longest] = (place[longest] + 1) % shape[longest]
    return drawn.at[tuple(place)].set(largest)


def strengthened(result, key, source, target, blocks, factor):
    owner, partner = [(jnp.arange(result.shape[axis_at]) // (result.shape[axis_at] // blocks)).reshape([-1 if axis == axis_at else 1 for axis in range(result.ndim)]) for axis_at in (source, target)]
    chosen = jax.random.permutation(key, blocks)[partner]
    strong = (owner == chosen) | (owner == (partner + blocks // 2) % blocks)
    return jnp.where(strong, factor * result, result)


def levels(stream_key, dims, cuts, low, top_value):
    def one(position, shards_of):
        heights = jax.random.uniform(jax.random.fold_in(jax.random.fold_in(stream_key, 6), position), (shards_of,), jnp.float32, low / len(cuts), top_value / len(cuts))
        return jnp.repeat(jnp.exp(heights), dims[position] // shards_of).reshape((-1,) + (1,) * (len(dims) - position - 1))

    level = one(*cuts[0])
    for cut in cuts[1:]:
        level = level * one(*cut)
    return level


def centred(rng, shape, deviation, limit, cuts=(), kind=jnp.bfloat16):
    level = levels(rng, shape, cuts, -0.22, 0.18) if cuts else 1.0
    values = jax.random.normal(rng, shape, jnp.float32) * deviation * level
    return jnp.minimum(jnp.maximum(values, -limit), limit).astype(kind)


def noise_with(own_key, shape, scale, bound, pieces, heavy, kind=jnp.bfloat16):
    entries = scale * jax.random.normal(own_key, shape, jnp.float32)
    if pieces:
        entries = entries * levels(own_key, shape, pieces, -0.22, 0.18)
    return jnp.clip(strengthened(entries, jax.random.fold_in(own_key, 3), *heavy), -bound, bound).astype(kind)


def setup_inputs(seed: int = 0) -> dict:
    streams_of = jax.random.split(jax.random.key(seed), 8)
    activations = noise_with(streams_of[0], (TOKENS, FF), 1.0, 6.0, ((0, 16), (1, 2)), (0, 1, 16, 2.0))
    output_gradient = centred(streams_of[1], (TOKENS, D), 1.0, 6.0, ((0, 16), (1, 2)))
    adapter_a = centred(streams_of[2], (TP_BLOCKS, FF_TP, R), FF ** -0.5, 0.0390625, ((0, 2), (1, 16)))
    adapter_b = centred(streams_of[3], (R, D), D ** -0.5, 0.078125, ((1, 2),))
    log_ratio = centred(streams_of[4], (TOKENS,), 0.25, 1.5, ((0, 16),), jnp.float32)
    lengths = draw_lengths(jax.random.fold_in(streams_of[7], 71), 0)
    rewards = with_ends(jax.random.randint(streams_of[6], (GROUPS, ROLLOUTS), 0, 11), jax.random.fold_in(streams_of[6], 1), 0, 10).astype(jnp.int32)
    return dict(activations=activations, output_gradient=output_gradient, adapter_a=adapter_a, adapter_b=adapter_b, log_ratio=log_ratio, lengths=lengths, rewards=rewards)


clip_eps = 0.2
adapter_scale_factor = 2.0

def token_terms(length_row, reward_row, log_ratio, offset):
    reward = reward_row.astype(jnp.float32)
    center = jnp.mean(reward)
    spread = jnp.mean((reward - center) * (reward - center))
    advantage = (reward - center) / jnp.sqrt(spread + 1.0)
    ends = jnp.cumsum(length_row).astype(jnp.int32)
    starts = (ends - length_row).astype(jnp.int32)
    slots = jnp.arange(log_ratio.shape[0], dtype=jnp.int32) + offset
    member = ((slots[None, :] >= starts[:, None]) & (slots[None, :] < ends[:, None])).astype(jnp.float32)
    live = lax.optimization_barrier(jnp.sum(member, axis=0))
    token_adv = lax.optimization_barrier(jnp.sum(member * advantage[:, None], axis=0))
    ratio = jnp.exp(log_ratio)
    unclipped = ratio * token_adv
    clipped = jnp.clip(ratio, 1.0 - clip_eps, 1.0 + clip_eps) * token_adv
    token_loss = -jnp.minimum(unclipped, clipped)
    slope = jnp.where(unclipped <= clipped, -unclipped, jnp.zeros_like(unclipped))
    return (live * slope, jnp.sum(live * token_loss), jnp.sum(live))

def reference(activations, output_gradient, adapter_a, adapter_b, log_ratio, lengths, rewards):
    groups = lengths.shape[0]
    offsets = jnp.zeros((groups,), jnp.int32)
    token_coefficient, loss_parts, live_parts = jax.vmap(token_terms)(lengths, rewards, log_ratio.reshape(groups, -1), offsets)
    token_coefficient = token_coefficient.reshape(-1)
    ratio_multiplier = groups / jnp.sum(live_parts)
    a_whole = adapter_a.reshape(-1, adapter_a.shape[2])
    low_rank = jnp.dot(activations, a_whole, preferred_element_type=jnp.float32)
    backward_projection = jnp.dot(output_gradient, adapter_b.T, preferred_element_type=jnp.float32)
    error_rows = (adapter_scale_factor * token_coefficient[:, None] * backward_projection).astype(jnp.bfloat16)
    grad_a = ratio_multiplier * lax.dot_general(activations, error_rows, (((0,), (0,)), ((), ())), preferred_element_type=jnp.float32)
    weighted_error = token_coefficient[:, None] * low_rank
    adapter_b_gradient = ratio_multiplier * adapter_scale_factor * jnp.dot(weighted_error.T, output_gradient.astype(jnp.float32), precision=lax.Precision.HIGHEST)
    loss = ratio_multiplier * jnp.sum(loss_parts)
    return (grad_a.reshape(adapter_a.shape), adapter_b_gradient, loss)
```

```python
import functools

import jax
import jax.numpy as jnp
from jax import lax
from jax.experimental import pallas as pl
from jax.experimental.pallas import tpu as pltpu
from jax.sharding import PartitionSpec as P

clip_eps = 0.2
adapter_scale_factor = 2.0


def token_terms(length_row, reward_row, log_ratio, offset):
    reward = reward_row.astype(jnp.float32)
    center = jnp.mean(reward)
    spread = jnp.mean((reward - center) * (reward - center))
    advantage = (reward - center) / jnp.sqrt(spread + 1.0)
    ends = jnp.cumsum(length_row)
    starts = ends - length_row
    slots = jnp.arange(log_ratio.shape[0], dtype=jnp.int32) + offset
    member = ((slots[None, :] >= starts[:, None]) & (slots[None, :] < ends[:, None])).astype(
        jnp.float32
    )
    live = jnp.sum(member, axis=0)
    token_adv = jnp.sum(member * advantage[:, None], axis=0)
    ratio = jnp.exp(log_ratio)
    unclipped = ratio * token_adv
    clipped = jnp.clip(ratio, 1.0 - clip_eps, 1.0 + clip_eps) * token_adv
    token_loss = -jnp.minimum(unclipped, clipped)
    slope = jnp.where(unclipped <= clipped, -unclipped, jnp.zeros_like(unclipped))
    return (live * slope, jnp.sum(live * token_loss), jnp.sum(live))


def plain_local(activations, output_gradient, adapter_a, adapter_b, log_ratio, lengths, rewards):
    tokens = activations.shape[0]
    groups = lengths.shape[0]
    per_group = lax.axis_size("dp") // groups
    position = lax.axis_index("dp")
    group_id = position // per_group
    offset = position % per_group * tokens
    length_row = lax.dynamic_index_in_dim(lengths, group_id, 0, keepdims=False)
    reward_row = lax.dynamic_index_in_dim(rewards, group_id, 0, keepdims=False)
    token_coefficient, loss_local, live_count = token_terms(
        length_row, reward_row, log_ratio, offset
    )
    columns = activations
    partial_low = jnp.dot(
        columns,
        lax.all_gather(adapter_a, "dp", axis=1, tiled=True)[0],
        preferred_element_type=jnp.float32,
    )
    partial_back = lax.dot_general(
        output_gradient, adapter_b, (((1,), (1,)), ((), ())), preferred_element_type=jnp.float32
    )
    low_rank, backward_projection = lax.psum((partial_low, partial_back), "tensor")
    error_rows = (adapter_scale_factor * token_coefficient[:, None] * backward_projection).astype(
        jnp.bfloat16
    )
    weighted_error = token_coefficient[:, None] * low_rank
    local_adapter_b_gradient = adapter_scale_factor * jnp.einsum(
        "tr,td->rd",
        weighted_error,
        output_gradient.astype(jnp.float32),
        precision=lax.Precision.HIGHEST,
    )
    columns = activations
    grad_a = lax.psum_scatter(
        lax.dot_general(
            columns, error_rows, (((0,), (0,)), ((), ())), preferred_element_type=jnp.float32
        ),
        "dp",
        scatter_dimension=0,
        tiled=True,
    )
    grad_b_sum, loss_sum, live_sum = lax.psum(
        (local_adapter_b_gradient, loss_local, live_count), "dp"
    )
    factor = groups / live_sum
    return ((factor * grad_a)[None], factor * grad_b_sum, factor * loss_sum)


MESH = pl.DeviceIdType.MESH
f32, bf16 = jnp.float32, jnp.bfloat16


def tile_of(total, most):
    return max(k for k in range(128, most + 1, 128) if total % k == 0)


def fused_kernel(
    n, groups, rollouts,
    act_hbm, grad_hbm, a_hbm, b_hbm, ratio_ref, len_ref, rew_ref,
    out_a, out_b, out_loss,
    act, grad, b_mat, a_all, part, rs1, rs2, rs3, xs, xr, coef, err,
    gb, gbs, gb1, gb2s, gb2, gb3s, gb3, fin, ls, l1, l2, lz,
    loc, ag_s, ag_r, rs1_s, rs1_r, rs2_s, rs2_r, rs3_s, rs3_r, x_s, x_r,
    g_s, g_r, gz_s, gz_r, fz_s, fz_r, l_s, l_r, lz_s, lz_r,
):
    depth = n // 4
    p = lax.axis_index("dp")
    t = lax.axis_index("tensor")
    c, y, z = p % 2, (p // 2) % 2, p // 4
    tokens, ff = act.shape
    rows, rank = a_hbm.shape

    def at(zz, yy, cc):
        return (zz * 2 + yy) * 2 + cc

    def turn(k):
        return lax.rem(z + (k + depth), depth)

    def block(ref, q):
        return ref.at[pl.ds(pl.multiple_of(q * rows, 16), rows)]

    def remote(s, d, ss, rs, dev, tensor=None):
        return pltpu.make_async_remote_copy(
            src_ref=s, dst_ref=d, send_sem=ss, recv_sem=rs,
            device_id=(dev, t if tensor is None else tensor), device_id_type=MESH,
        )

    core, side = at(z, y, 1 - c), at(z, 1 - y, c)
    zs = [turn(k) for k in range(depth)]
    peer = [at(zs[k], y, c) for k in range(depth)]

    load_a = pltpu.make_async_copy(a_hbm, block(a_all, p), loc.at[0])
    load_g = pltpu.make_async_copy(grad_hbm, grad, loc.at[1])
    load_b = pltpu.make_async_copy(b_hbm, b_mat, loc.at[2])
    load_x = pltpu.make_async_copy(act_hbm, act, loc.at[3])
    for copy in (load_a, load_g, load_b, load_x):
        copy.start()

    barrier = pltpu.get_barrier_semaphore()
    for dev in [core, side] + peer[1:]:
        pl.semaphore_signal(barrier, inc=1, device_id=(dev, t), device_id_type=MESH)
    pl.semaphore_signal(barrier, inc=1, device_id=(p, 1 - t), device_id_type=MESH)
    pl.semaphore_wait(barrier, depth + 2)

    sent = []

    def go(copy):
        copy.start()
        sent.append(copy)
        return copy

    count = [0]

    def gather_send(q, dev):
        go(remote(block(a_all, q), block(a_all, q), ag_s.at[count[0]], ag_r.at[q], dev))
        count[0] += 1

    def gather_wait(q):
        remote(block(a_all, q), block(a_all, q), ag_s.at[0], ag_r.at[q], core).wait_recv()

    load_a.wait()
    far = sorted(range(1, depth), key=lambda k: -min(k, depth - k))
    gather_send(p, side)
    for k in far:
        gather_send(p, peer[k])
    gather_send(p, core)

    load_g.wait()
    load_b.wait()
    xs[0] = lax.dot_general(grad[...], b_mat[...], (((1,), (1,)), ((), ())), preferred_element_type=f32)
    back = go(remote(xs.at[0], xr.at[0], x_s.at[0], x_r.at[0], p, 1 - t))

    per_group = n // groups
    group = p // per_group
    offset = (p % per_group) * tokens
    slots = (
        lax.broadcasted_iota(jnp.int32, ratio_ref.shape, 0) * 128
        + lax.broadcasted_iota(jnp.int32, ratio_ref.shape, 1)
        + offset
    )
    live_total = jnp.int32(0)
    live = jnp.zeros(ratio_ref.shape, f32)
    token_adv = jnp.zeros(ratio_ref.shape, f32)
    for g in range(groups):
        here = jnp.full((1, 128), (group == g).astype(f32))
        reward = [jnp.full((1, 128), rew_ref[g, i]).astype(f32) for i in range(rollouts)]
        center = sum(reward) / rollouts
        spread = sum((r - center) * (r - center) for r in reward) / rollouts
        scale = jnp.sqrt(spread + 1.0)
        end = jnp.int32(0)
        for i in range(rollouts):
            start = end
            end = end + len_ref[g, i]
            member = ((slots >= start) & (slots < end)).astype(f32) * here
            live = live + member
            token_adv = token_adv + member * ((reward[i] - center) / scale)
        live_total = live_total + jnp.minimum(end, per_group * tokens)
    ratio = jnp.exp(ratio_ref[...])
    unclipped = ratio * token_adv
    clipped = jnp.clip(ratio, 1.0 - clip_eps, 1.0 + clip_eps) * token_adv
    token_loss = -jnp.minimum(unclipped, clipped)
    slope = jnp.where(unclipped <= clipped, -unclipped, jnp.zeros_like(unclipped))
    weight = live * slope
    for i in range(tokens // 128):
        coef[pl.ds(i * 128, 128), :] = jnp.broadcast_to(weight[i : i + 1, :], (128, 128)).T
    factor = groups / jnp.full((1, 128), live_total).astype(f32)
    loss_part = jnp.sum(jnp.sum(live * token_loss, axis=1, keepdims=True), axis=0, keepdims=True)

    ls[0] = jnp.broadcast_to(loss_part, (8, 128))
    first = go(remote(ls.at[0], l1, l_s.at[0], l_r.at[0], core))

    back.wait_recv()
    err[...] = (adapter_scale_factor * coef[...] * (xs[0] + xr[0])).astype(bf16)

    load_x.wait()
    tile = tile_of(ff, 1536)
    steps = ff // tile

    def partial_rows(i, _):
        cols = pl.ds(pl.multiple_of(i * tile, 128), tile)
        part[cols, :] = lax.dot_general(
            act[:, cols], err[...], (((0,), (0,)), ((), ())), preferred_element_type=f32
        ).astype(bf16)
        return 0

    near = [depth - k for k in far][::-1]
    for j, k in enumerate(near):
        lax.fori_loop(j * steps // len(near), (j + 1) * steps // len(near), partial_rows, 0)
        q = peer[k]
        gather_wait(q)
        gather_send(q, side)
        gather_send(q, core)

    order = far + [0]
    first_stage = {}
    for yy in (1, 0):
        for k in order:
            yv = 1 - y if yy else y
            i = k * 2 + yy
            first_stage[k, yy] = go(
                remote(block(part, at(zs[k], yv, 1 - c)), rs1.at[i], rs1_s.at[i], rs1_r.at[i], core)
            )

    first.wait_recv()
    ls[1] = ls[0] + l1[...]
    second = go(remote(ls.at[1], l2, l_s.at[1], l_r.at[1], side))

    second_stage = {}
    for k in order:
        first_stage[k, 1].wait_recv()
        own = block(part, at(zs[k], 1 - y, c))
        own[...] = (own[...].astype(f32) + rs1[k * 2 + 1].astype(f32)).astype(bf16)
        second_stage[k] = go(remote(own, rs2.at[k], rs2_s.at[k], rs2_r.at[k], side))

    second.wait_recv()
    lz[z] = ls[1] + l2[...]
    third = [go(remote(lz.at[z], lz.at[z], lz_s.at[k], lz_r.at[k], peer[k])) for k in range(1, depth)]

    for k in [0] + near:
        q = at(zs[k], 1 - y, c)
        gather_wait(q)
        gather_send(q, core)
    for k in range(depth):
        gather_wait(at(zs[k], y, 1 - c))
    for k in range(depth):
        gather_wait(at(zs[k], 1 - y, 1 - c))

    def low_rows(i, total):
        cols = pl.ds(pl.multiple_of(i * tile, 128), tile)
        return total + jnp.dot(act[:, cols], a_all[cols, :], preferred_element_type=f32)

    xs[1] = lax.fori_loop(0, steps, low_rows, jnp.zeros((tokens, rank), f32))
    low = go(remote(xs.at[1], xr.at[1], x_s.at[1], x_r.at[1], p, 1 - t))

    third_stage = {}
    for k in far:
        first_stage[k, 0].wait_recv()
        second_stage[k].wait_recv()
        own = block(part, at(zs[k], y, c))
        own[...] = (
            own[...].astype(f32) + rs1[k * 2].astype(f32) + rs2[k].astype(f32)
        ).astype(bf16)
        third_stage[k] = go(remote(own, rs3.at[k], rs3_s.at[k], rs3_r.at[k], peer[k]))

    low.wait_recv()
    weighted = coef[...] * (xs[1] + xr[1])
    high = weighted.astype(bf16)
    rest = weighted - high.astype(f32)
    middle = rest.astype(bf16)
    last = (rest - middle.astype(f32)).astype(bf16)
    width = grad.shape[1]
    wide = tile_of(width, 640)
    for i in range(width // wide):
        cols = pl.ds(i * wide, wide)
        g = grad[:, cols]
        total = sum(
            lax.dot_general(w, g, (((0,), (0,)), ((), ())), preferred_element_type=f32)
            for w in (last, middle, high)
        )
        gb[:, cols] = total
        gbs[:, cols] = total.astype(bf16)

    half, quarter, chunk = rank // 2, rank // 4, width // depth
    lane = pl.multiple_of(c * half, 16)
    other = pl.multiple_of((1 - c) * half, 16)
    one = go(remote(gbs.at[pl.ds(other, half)], gb1, g_s.at[0], g_r.at[0], core))
    one.wait_recv()
    away = pl.multiple_of((1 - y) * quarter, 16)
    stay = pl.multiple_of(y * quarter, 16)
    mine = pl.multiple_of(lane + stay, 16)
    gb2s[...] = (
        gb[pl.ds(pl.multiple_of(lane + away, 16), quarter), :] + gb1[pl.ds(away, quarter), :].astype(f32)
    ).astype(bf16)
    two = go(remote(gb2s, gb2, g_s.at[1], g_r.at[1], side))

    first_stage[0, 0].wait_recv()
    second_stage[0].wait_recv()
    total = block(part, p)[...].astype(f32) + rs1[0].astype(f32) + rs2[0].astype(f32)
    out_a[...] = total

    two.wait_recv()
    total = (
        gb[pl.ds(mine, quarter), :]
        + gb1[pl.ds(stay, quarter), :].astype(f32)
        + gb2[...].astype(f32)
    )
    gb3s[...] = total.astype(bf16)
    gb[pl.ds(mine, quarter), :] = total

    def chunk_of(zz):
        return pl.ds(pl.multiple_of(zz * chunk, 128), chunk)

    three = {
        k: go(remote(gb3s.at[:, chunk_of(zs[k])], gb3.at[k], gz_s.at[k], gz_r.at[k], peer[k]))
        for k in far
    }

    for k in far:
        third_stage[k].wait_recv()
        out_a[...] = out_a[...] + rs3[k].astype(f32)
    out_a[...] = factor * out_a[...]
    for copy in third:
        copy.wait_recv()
    total = lz[0]
    for i in range(1, depth):
        total = total + lz[i]
    out_loss[...] = factor * total

    for k in far:
        three[k].wait_recv()
    total = gb[pl.ds(mine, quarter), chunk_of(z)]
    for k in far:
        total = total + gb3[k].astype(f32)
    scaled = jnp.full((1, 128), adapter_scale_factor) * factor
    fin[pl.ds(mine, quarter), chunk_of(z)] = (scaled[:, :1] * total).astype(bf16)

    piece = fin.at[pl.ds(mine, quarter), chunk_of(z)]
    four = {k: go(remote(piece, piece, fz_s.at[k], fz_r.at[k], peer[k])) for k in far}
    for k in far:
        four[k].wait_recv()
    piece = fin.at[pl.ds(mine, quarter)]
    five = go(remote(piece, piece, g_s.at[2], g_r.at[2], side))
    five.wait_recv()
    piece = fin.at[pl.ds(lane, half)]
    six = go(remote(piece, piece, g_s.at[3], g_r.at[3], core))
    six.wait_recv()
    out_b[...] = fin[...].astype(f32)
    for copy in sent:
        copy.wait_send()


def fused_local(activations, output_gradient, adapter_a, adapter_b, log_ratio, lengths, rewards):
    n = lax.axis_size("dp")
    depth = n // 4
    tokens, ff = activations.shape
    rows, rank = adapter_a.shape[1:]
    width = output_gradient.shape[1]
    dma = pltpu.SemaphoreType.DMA
    vmem, anywhere = pl.BlockSpec(memory_space=pltpu.VMEM), pl.BlockSpec(memory_space=pl.ANY)
    scalars = pl.BlockSpec(memory_space=pltpu.SMEM)
    quarter, chunk = rank // 4, width // depth
    grad_a, grad_b, loss = pl.pallas_call(
        functools.partial(fused_kernel, n, lengths.shape[0], lengths.shape[1]),
        out_shape=(
            jax.ShapeDtypeStruct((rows, rank), f32),
            jax.ShapeDtypeStruct((rank, width), f32),
            jax.ShapeDtypeStruct((8, 128), f32),
        ),
        in_specs=[anywhere] * 4 + [vmem, scalars, scalars],
        out_specs=(vmem, vmem, vmem),
        scratch_shapes=[
            pltpu.VMEM((tokens, ff), bf16),
            pltpu.VMEM((tokens, width), bf16),
            pltpu.VMEM((rank, width), bf16),
            pltpu.VMEM((ff, rank), bf16),
            pltpu.VMEM((ff, rank), bf16),
            pltpu.VMEM((2 * depth, rows, rank), bf16),
            pltpu.VMEM((depth, rows, rank), bf16),
            pltpu.VMEM((depth, rows, rank), bf16),
            pltpu.VMEM((2, tokens, rank), f32),
            pltpu.VMEM((2, tokens, rank), f32),
            pltpu.VMEM((tokens, rank), f32),
            pltpu.VMEM((tokens, rank), bf16),
            pltpu.VMEM((rank, width), f32),
            pltpu.VMEM((rank, width), bf16),
            pltpu.VMEM((rank // 2, width), bf16),
            pltpu.VMEM((quarter, width), bf16),
            pltpu.VMEM((quarter, width), bf16),
            pltpu.VMEM((quarter, width), bf16),
            pltpu.VMEM((depth, quarter, chunk), bf16),
            pltpu.VMEM((rank, width), bf16),
            pltpu.VMEM((2, 8, 128), f32),
            pltpu.VMEM((8, 128), f32),
            pltpu.VMEM((8, 128), f32),
            pltpu.VMEM((depth, 8, 128), f32),
            dma((4,)), dma((n - 1 + 0,)), dma((n,)),
            dma((2 * depth,)), dma((2 * depth,)),
            dma((depth,)), dma((depth,)), dma((depth,)), dma((depth,)),
            dma((2,)), dma((2,)),
            dma((4,)), dma((4,)), dma((depth,)), dma((depth,)), dma((depth,)), dma((depth,)),
            dma((2,)), dma((2,)), dma((depth,)), dma((depth,)),
        ],
        compiler_params=pltpu.CompilerParams(
            collective_id=0, has_side_effects=True, vmem_limit_bytes=48 * 1024 * 1024
        ),
        name="fused",
    )(
        activations, output_gradient, adapter_a[0], adapter_b,
        log_ratio.reshape(-1, 128), lengths, rewards,
    )
    return grad_a[None], grad_b, loss[0, 0]


def fits(mesh):
    n, split = mesh.shape["dp"], mesh.shape["tensor"]
    return n % 4 == 0 and 4 <= n <= 16 and split == 2


def local(activations, output_gradient, adapter_a, adapter_b, log_ratio, lengths, rewards):
    n = lax.axis_size("dp")
    rows, rank = adapter_a.shape[1:]
    width, ff = output_gradient.shape[1], activations.shape[1]
    small = 2 * activations.size + 8 * ff * rank < 32 * 1024 * 1024
    aligned = (
        rows % 16 == 0
        and rank == 128
        and activations.shape[0] % 128 == 0
        and ff % 128 == 0
        and width % (128 * (n // 4)) == 0
        and n % lengths.shape[0] == 0
    )
    run = fused_local if small and aligned else plain_local
    return run(activations, output_gradient, adapter_a, adapter_b, log_ratio, lengths, rewards)


def solution(mesh):
    in_specs = (
        P("dp", "tensor"),
        P("dp", "tensor"),
        P("tensor", "dp", None),
        P(None, "tensor"),
        P("dp"),
        P(),
        P(),
    )
    out_specs = (P("tensor", "dp", None), P(None, "tensor"), P())
    body = local if fits(mesh) else plain_local
    return jax.shard_map(body, mesh=mesh, in_specs=in_specs, out_specs=out_specs, check_vma=False)
```
